128 devices in a mesh: grp: 4 (over z_hi, core), own: 32 (over z_lo, x, y).
Axes of the slice: x: 4, y: 4, z: 4 (z_hi: 2, z_lo: 2; z = z_hi * 2 + z_lo), core: 2. Of those that a mesh axis runs over, the one named last changes fastest.
Arguments:
- features: float32 [131072, 1024], P(('grp', 'own')), may hold values from -9 to 9, as said below
- targets: float32 [131072, 256], P(('grp', 'own')), may hold values from -6 to 6
- centres: float32 [4096, 1024], P('own'), may hold values from -6 to 6
- widths: float32 [4096], P('own'), may hold values from 256 to 1024
- coefficients: float32 [4096, 256], P('own'), may hold values from -0.375 to 0.375
Outputs:
- residual: float32 [131072, 256], P(('grp', 'own'))
- gradient: float32 [4096, 256], P('own')
The draws below stay inside these ranges and needn't reach their ends.
Inputs may be any that keep to these rules, and one draw needn't show every extreme that they name: Every row of features lies near one of the centres; which centre it is is not promised.
All inputs are finite; a program needn't handle non-finite values.
Results may differ from the reference program's by a relative error of at most 0.00015.
Values sent between devices are 32-bit elements; how exact they have to be, the bound alone decides.
A program may use at most 128 MiB of HBM per device.

```python
import math
import jax
import jax.numpy as jnp
from jax import lax

D = 1024
TGT = 256
ROWS_DEV = 1024
CEN_DEV = 128
TOTAL = 131072
CENTRES = 4096
N_OWN = 32


def clustered(key):
    centres = jnp.clip(jax.random.normal(jax.random.fold_in(key, 11), (CENTRES, D), jnp.float32), -6.0, 6.0)
    picks = jax.random.randint(jax.random.fold_in(key, 12), (TOTAL,), 0, CENTRES)
    noise = jnp.clip(0.5 * jax.random.normal(jax.random.fold_in(key, 13), (TOTAL, D), jnp.float32), -3.0, 3.0)
    return (centres, centres[picks] + noise)


def draw_features(key, part):
    return clustered(key)[1]


def draw_centres(key, part):
    return clustered(key)[0]


def shard_levels(own_key, dims, shards, low, high):
    loudness, own = 1.0, jax.random.fold_in(own_key, 6)
    for dim, shards_of in shards:
        heights = jnp.exp(jax.random.uniform(jax.random.fold_in(own, dim), (shards_of,), jnp.float32, low / len(shards), high / len(shards)))
        loudness = loudness * jnp.repeat(heights, dims[dim] // shards_of).reshape([-1 if axis == dim else 1 for axis in range(len(dims))])
    return loudness


def scatter_about(rng, extent, deviation, reach, split=(), kind=jnp.bfloat16):
    factor_of = shard_levels(rng, extent, split, -0.22, 0.18) if split else 1.0
    entries = jax.random.normal(rng, extent, jnp.float32) * deviation * factor_of
    return jnp.minimum(jnp.maximum(entries, -reach), reach).astype(kind)


def setup_inputs(seed: int = 0) -> dict:
    arg_keys = jax.random.split(jax.random.key(seed), 6)
    features = draw_features(jax.random.fold_in(arg_keys[5], 71), 0)
    targets = scatter_about(arg_keys[1], (TOTAL, TGT), 1.0, 6.0, ((0, 128),), jnp.float32)
    centres = draw_centres(jax.random.fold_in(arg_keys[5], 71), 0)
    widths = jnp.clip(jnp.exp(math.log(1024.0) - 1.3862944 * jax.random.uniform(arg_keys[3], (CENTRES,), jnp.float32) ** shard_levels(arg_keys[3], (CENTRES,), ((0, 32),), -0.2, 0.2)), 256.0, 1024.0)
    coefficients = scatter_about(arg_keys[4], (CENTRES, TGT), (CEN_DEV * N_OWN // 16) ** -0.5, 0.375, ((0, 32),), jnp.float32)
    return dict(features=features, targets=targets, centres=centres, widths=widths, coefficients=coefficients)


def kernel_block(rows, centres, widths):
    cross = jnp.dot(rows, centres.T, precision=lax.Precision.HIGHEST, preferred_element_type=jnp.float32)
    row_sq = lax.optimization_barrier(jnp.sum(rows * rows, axis=1))
    cen_sq = lax.optimization_barrier(jnp.sum(centres * centres, axis=1))
    sq_dist = row_sq[:, None] + cen_sq[None, :] - 2.0 * cross
    return jnp.exp(-sq_dist / (2.0 * widths[None, :]))

def reference(features, targets, centres, widths, coefficients):
    blocks = features.shape[0] // ROWS_DEV
    row_blocks = features.reshape(blocks, ROWS_DEV, features.shape[1])
    tgt_blocks = targets.reshape(blocks, ROWS_DEV, targets.shape[1])

    def step(carry, pair):
        rows, tgt = pair
        kern = kernel_block(rows, centres, widths)
        pred = jnp.dot(kern, coefficients, precision=lax.Precision.HIGHEST, preferred_element_type=jnp.float32)
        resid = pred - tgt
        term = jnp.dot(kern.T, resid, precision=lax.Precision.HIGHEST, preferred_element_type=jnp.float32)
        return (carry + term, resid)
    start = jnp.zeros(coefficients.shape, jnp.float32)
    total, resids = lax.scan(step, start, (row_blocks, tgt_blocks))
    residual = resids.reshape(targets.shape)
    gradient = total / jnp.sqrt(jnp.float32(features.shape[0]))
    return (residual, gradient)
```

```python
import functools
import math
import jax
import jax.numpy as jnp
from jax import lax
from jax.experimental import pallas as pl
from jax.experimental.pallas import tpu as pltpu
from jax.sharding import PartitionSpec as P

F32, BF16, F8 = jnp.float32, jnp.bfloat16, jnp.float8_e4m3fn
NN = (((1,), (0,)), ((), ()))
NT = (((1,), (1,)), ((), ()))
MESH = pl.DeviceIdType.MESH

PIECE = 32
CHUNK = 256
UNITS = 64
DIRS = ("d1+", "d1-", "d2+", "d2-", "z+", "z-")


def messages():
    out = []

    def add(*m):
        out.append(m)

    for r1 in range(4):
        b = (0, r1, 0)
        if r1 == 0:
            add(0, b, (0, 3, 0), None, "d1+")
            add(0, b, (0, 1, 0), None, "d1-")
        if r1 == 3:
            add(0, b, (0, 2, 0), 0, "d1+")
        if r1 == 1:
            add(0, b, (0, 2, 0), 1, "d1-")
        add(0, b, (0, r1, 3), None, "d2+")
        add(0, b, (0, r1, 1), None, "d2-")
        add(0, (0, r1, 3), (0, r1, 2), 0, "d2+")
        add(0, (0, r1, 1), (0, r1, 2), 1, "d2-")
    for r1 in range(4):
        for r2 in range(4):
            add(0, (0, r1, r2), (1, r1, r2), None, "z+" if (r1 + r2) % 2 == 0 else "z-")
    b = (0, 0, 0)
    add(1, b, (0, 0, 3), None, "d2+")
    add(1, b, (0, 0, 1), None, "d2-")
    add(1, (0, 0, 3), (0, 0, 2), 0, "d2+")
    add(1, (0, 0, 1), (0, 0, 2), 1, "d2-")
    for r2 in range(4):
        add(1, (0, 0, r2), (1, 0, r2), None, "z-" if r2 % 2 == 0 else "z+")
    for rz in range(2):
        for r2 in range(4):
            s = (rz, 0, r2)
            add(1, s, (rz, 3, r2), None, "d1+")
            add(1, s, (rz, 1, r2), None, "d1-")
            add(1, (rz, 3, r2), (rz, 2, r2), 0, "d1+")
            add(1, (rz, 1, r2), (rz, 2, r2), 1, "d1-")
    return out


FIRST = (0, 1, 36, 37, 2, 3, 40, 44, 45, 20)
SCHEDULE = (
    ((0, (15, 16, 17, 32)), (1, (6, 7, 8, 24)), (20, ()), (36, (38, 43, 56, 57)), (37, (39, 41, 48, 49)), (40, (60, 61))),
    (),
    ((2, (4, 23)), (3, (5, 21)), (44, (46,)), (45, (47,))),
    ((6, ()), (15, (11, 12, 28)), (32, ()), (43, (72, 73)), (16, (18, 35))),
    ((17, (19, 33)), (56, (58,)), (57, (59,)), (24, ()), (41, (64, 65))),
    ((7, (9, 27)), (8, (10, 25))),
    ((38, ()), (39, (42, 52, 53))),
    ((48, (50,)), (49, (51,)), (23, ()), (28, ()), (4, ()), (5, (22,))),
    ((60, (62,)), (61, (63,)), (21, ()), (35, ())),
    (),
    ((11, (13, 31)), (12, (14, 29)), (46, ()), (47, ())),
    ((18, ()), (19, (34,)), (33, ()), (42, (68, 69))),
    ((9, ()), (10, (26,))),
    ((72, (74,)), (73, (75,)), (13, ()), (14, (30,)), (58, ()), (59, ()), (27, ())),
    ((31, ()), (64, (66,)), (65, (67,))),
    (),
    ((52, (54,)), (53, (55,)), (25, ()), (50, ()), (51, ())),
    ((29, ()), (62, ()), (63, ())),
    ((68, (70,)), (69, (71,))),
    ((22, ()), (74, ()), (75, ()), (34, ()), (66, ()), (67, ())),
    ((54, ()), (55, ()), (70, ()), (71, ()), (30, ())),
    ((26, ()),),
    (),
    (),
)

STEPS = len(SCHEDULE) // 8 - 1
MSGS = messages()


def unit_order():
    place = {(0, (0, 0, 0)): 0, (1, (0, 0, 0)): 1}
    halves = {}
    for point in SCHEDULE:
        for m, _ in point:
            part, _, dst, half, _ = MSGS[m]
            seen = halves.setdefault((part, dst), set())
            seen.update((0, 1) if half is None else (half,))
            if len(seen) == 2:
                place[(part, dst)] = len(place)
    return place


PLACE = unit_order()
UNIT_AT = {v: k for k, v in PLACE.items()}
LOG2E = 1.4426950408889634
S_HI, S_LO = 4.0, 1024.0
S_K, S_KLO = 16.0, 4096.0
S_C, S_CLO = 64.0, 16384.0
S_R, S_RLO = 0.25, 64.0


def dot(a, b, dims):
    return lax.dot_general(a, b, dims, preferred_element_type=F32)


def split(v):
    hi = v.astype(BF16)
    return hi, v - hi.astype(F32)


def main_kernel(
    feat, targ, cent, wid, coef, resid, grad,
    CB, WV, FS, FH, FX, RS, CH, CX, WH, WX, MB, KH, KX, PRED, TG, PR, RES, RP,
    RTH, RTL, RTR, GT, G0, G1, GO,
    ra0, rb0, sa0, sb0, ta0, tb0, ra1, rb1, sa1, sb1, ta1, tb1,
    in_sem, own_sem, d_send, d_recv, g_send, g_recv, r_send, r_recv, f_send, f_recv, out_sem,
):
    rows, depth = feat.shape
    blocks = depth // 128
    unit_rows = CB.shape[1]
    tile = rows // 2
    wide = TG.shape[1]
    lane_w = wide // 128

    grp, own = lax.axis_index("grp"), lax.axis_index("own")
    core, z_hi = lax.rem(grp, 2), grp // 2
    z, x, y = z_hi * 2 + own // 16, lax.rem(own // 4, 4), lax.rem(own, 4)

    def device(d1=0, d2=0, dz=0, dcore=0):
        nx = lax.rem(x + 4 + d1 * (1 - core) + d2 * core, 4)
        ny = lax.rem(y + 4 + d1 * core + d2 * (1 - core), 4)
        nz = lax.rem(z + 4 + dz, 4)
        nc = lax.rem(core + dcore, 2)
        return ((nz // 2) * 2 + nc, lax.rem(nz, 2) * 16 + nx * 4 + ny)

    near = {
        "d1+": device(d1=1), "d1-": device(d1=-1),
        "d2+": device(d2=1), "d2-": device(d2=-1),
        "z+": device(dz=1), "z-": device(dz=-1),
    }
    sibling = device(dcore=1)
    holders = (sibling, device(dz=2), device(dz=2, dcore=1))

    def remote(src, dst, send, recv, to):
        return pltpu.make_async_remote_copy(
            src_ref=src, dst_ref=dst, send_sem=send, recv_sem=recv, device_id=to, device_id_type=MESH
        )

    loads = []

    def load(src, dst):
        copy = pltpu.make_async_copy(src, dst, in_sem.at[len(loads)])
        copy.start()
        loads.append(copy)
        return copy

    load(wid, WV)
    for p in range(2):
        first = pl.multiple_of((core * 2 + p) * PIECE, PIECE)
        for b in range(blocks):
            load(
                cent.at[pl.ds(first, PIECE), pl.ds(b * 128, 128)],
                CB.at[p, pl.ds(b * PIECE, PIECE), :],
            )
        for b in range(lane_w):
            load(
                coef.at[pl.ds(first, PIECE), pl.ds(b * 128, 128)],
                CB.at[p, pl.ds((blocks + b) * PIECE, PIECE), :],
            )
    feat_in = pltpu.make_async_copy(feat, FS.at[0], own_sem.at[0])
    feat_in.start()
    targ_in = pltpu.make_async_copy(targ, TG, own_sem.at[1])
    targ_in.start()

    barrier = pltpu.get_barrier_semaphore()
    peers = list(near.values()) + list(holders)
    for to in peers:
        pl.semaphore_signal(barrier, inc=1, device_id=to, device_id_type=MESH)
    for copy in loads:
        copy.wait()

    row_i = lax.broadcasted_iota(jnp.int32, (PIECE, 128), 0)
    lane_i = lax.broadcasted_iota(jnp.int32, (PIECE, 128), 1)
    eye = (row_i == lane_i).astype(F32)
    meta_row = lax.broadcasted_iota(jnp.int32, (8, 128), 0)
    for p in range(2):
        sq = jnp.zeros((PIECE, 128), F32)
        for b in range(blocks):
            v = CB[p, b * PIECE : (b + 1) * PIECE, :]
            sq = sq + v * v
        norm = jnp.sum(sq, axis=1, keepdims=True)
        picked = jnp.where(lane_i == row_i + (core * 2 + p) * PIECE, WV[...], 0.0)
        width = jnp.sum(picked, axis=1, keepdims=True)
        scale = (-0.5 * LOG2E) / width
        norm = jnp.sum(norm * eye, axis=0, keepdims=True)
        scale = jnp.sum(scale * eye, axis=0, keepdims=True)
        CB[p, unit_rows - 8 : unit_rows, :] = jnp.where(
            meta_row == 0, scale, jnp.where(meta_row == 1, norm, 0.0)
        )
    pl.semaphore_wait(barrier, len(peers))

    cut = (unit_rows // 16) * 8
    spans = {None: (0, unit_rows), 0: (0, cut), 1: (cut, unit_rows - cut)}

    def message(m):
        part, src, dst, half, way = MSGS[m]
        at, size = spans[half]
        return remote(
            CB.at[PLACE[(part, src)], pl.ds(at, size), :],
            CB.at[PLACE[(part, dst)], pl.ds(at, size), :],
            g_send.at[m], g_recv.at[m], near[way],
        )

    def service(point):
        for m, onward in point:
            message(m).wait_recv()
            for n in onward:
                message(n).start()

    for m in FIRST:
        message(m).start()
    feat_out = remote(feat, FS.at[1], d_send.at[0], d_recv.at[0], sibling)
    feat_out.start()

    def prepare_rows(which):
        base = which * rows
        step = min(128, rows)

        @pl.loop(0, rows // step)
        def _(i):
            r = pl.multiple_of(i * step, step)
            v = FS[which, pl.ds(r, step), :]
            hi, lo = split(v)
            to = pl.ds(base + r, step)
            FH[to, :] = hi
            FX[to, 0:depth] = (v * S_HI).astype(F8)
            FX[to, depth : 2 * depth] = (lo * S_LO).astype(F8)
            RS[to, :] = jnp.broadcast_to(jnp.sum(v * v, axis=1, keepdims=True), (step, 128))

    def prepare_chunk(k):
        units = range(8 * k, 8 * k + 8)
        for b in range(blocks):
            v = jnp.concatenate([CB[u, b * PIECE : (b + 1) * PIECE, :] for u in units], axis=0)
            hi, lo = split(v)
            CH[:, b * 128 : (b + 1) * 128] = hi
            CX[:, b * 128 : (b + 1) * 128] = (lo * S_LO).astype(F8)
            CX[:, depth + b * 128 : depth + (b + 1) * 128] = (v * S_HI).astype(F8)
        for b in range(lane_w):
            at = (blocks + b) * PIECE
            v = jnp.concatenate([CB[u, at : at + PIECE, :] for u in units], axis=0)
            hi, lo = split(v)
            WH[:, b * 128 : (b + 1) * 128] = hi
            WX[0:CHUNK, b * 128 : (b + 1) * 128] = (lo * S_CLO).astype(F8)
            WX[CHUNK : 2 * CHUNK, b * 128 : (b + 1) * 128] = (v * S_C).astype(F8)
        for h in range(2):
            total = CB[8 * k + 4 * h, unit_rows - 8 : unit_rows, :]
            for j in range(1, 4):
                meta = CB[8 * k + 4 * h + j, unit_rows - 8 : unit_rows, :]
                total = total + pltpu.roll(meta, j * PIECE, 1)
            MB[:, h * 128 : (h + 1) * 128] = total

    def compute(k, base, n_tiles):
        def tile_body(i):
            r = pl.ds(pl.multiple_of(base + i * tile, tile), tile)
            cross = dot(FH[r, :], CH[...], NT)
            fine = dot(FX[r, :], CX[...], NT)
            norm = RS[r, :]
            norm = jnp.concatenate([norm, norm], axis=1)
            s = (norm + MB[1:2, :]) - 2.0 * cross - fine * (2.0 / (S_HI * S_LO))
            kern = jnp.exp2(s * MB[0:1, :])
            hi, lo = split(kern)
            KH[r, k * CHUNK : (k + 1) * CHUNK] = hi
            both = jnp.concatenate([(kern * S_K).astype(F8), (lo * S_KLO).astype(F8)], axis=1)
            KX[r, 2 * k * CHUNK : 2 * (k + 1) * CHUNK] = both
            term = dot(hi, WH[...], NN) + dot(both, WX[...], NN) * (1.0 / (S_K * S_CLO))
            if k == 0:
                PRED[r, :] = term
            else:
                PRED[r, :] = PRED[r, :] + term

        if n_tiles == 1:
            tile_body(0)
        else:
            pl.loop(0, n_tiles)(tile_body)

    feat_in.wait()
    prepare_rows(0)
    per_step = 4 // STEPS
    pred_out = [
        remote(
            PRED.at[pl.ds(rows + i * tile, tile), :], PR.at[pl.ds(i * tile, tile), :],
            d_send.at[1 + i], d_recv.at[1 + i], sibling,
        )
        for i in range(2)
    ]
    for k in range(8):
        service(SCHEDULE[k * (STEPS + 1)])
        prepare_chunk(k)
        for s in range(STEPS):
            at = s * per_step * tile
            if k == 7:
                at = lax.rem(at + rows, 2 * rows) if not isinstance(at, int) else (at + rows) % (2 * rows)
            if k == 0 and at == rows:
                feat_out.wait_recv()
                prepare_rows(1)
            compute(k, at, per_step)
            if k == 7 and at >= rows:
                for i in range(2):
                    if at <= rows + i * tile < at + per_step * tile:
                        pred_out[i].start()
            service(SCHEDULE[k * (STEPS + 1) + s + 1])

    def factors(v, at):
        t = v.T
        hi, lo = split(t)
        RTH[:, at : at + tile] = hi
        RTL[:, at : at + tile] = (lo * S_RLO).astype(F8)
        RTR[:, at : at + tile] = (t * S_R).astype(F8)

    targ_in.wait()
    res_out = []
    for i in range(2):
        part = pl.ds(i * tile, tile)
        pred_out[i].wait_recv()
        v = PRED[part, :] + PR[part, :] - TG[part, :]
        RES[part, :] = v
        copy = remote(RES.at[part, :], RP.at[part, :], d_send.at[3 + i], d_recv.at[3 + i], sibling)
        copy.start()
        res_out.append(copy)
        factors(v, i * tile)
    resid_out = pltpu.make_async_copy(RES, resid, out_sem.at[0])
    resid_out.start()

    def gradient_term(base, k):
        r = pl.ds(base, rows)
        if isinstance(k, int):
            c0, c1, c2 = k * CHUNK, 2 * k * CHUNK, (2 * k + 1) * CHUNK
        else:
            c0 = pl.multiple_of(k * CHUNK, CHUNK)
            c1 = pl.multiple_of(2 * k * CHUNK, CHUNK)
            c2 = pl.multiple_of((2 * k + 1) * CHUNK, CHUNK)
        term = dot(RTH[:, r], KH[r, pl.ds(c0, CHUNK)], NN)
        fine = dot(RTL[:, r], KX[r, pl.ds(c1, CHUNK)], NN) + dot(RTR[:, r], KX[r, pl.ds(c2, CHUNK)], NN)
        return term + fine * (1.0 / (S_RLO * S_K))

    @pl.loop(0, 8)
    def _(k):
        GT[k] = gradient_term(0, k)

    for i in range(2):
        res_out[i].wait_recv()
        factors(RP[i * tile : (i + 1) * tile, :], rows + i * tile)
    half_piece = PIECE // 2
    for k in range(8):
        t = (GT[k] + gradient_term(rows, k)).T
        for j in range(8):
            part, (rz, r1, r2) = UNIT_AT[8 * k + j]
            for h in range(2):
                at = j * PIECE + h * half_piece
                v = t[at : at + half_piece, :]
                if part == 0:
                    G0[rz, h, r2, r1] = v
                else:
                    G1[r1, r2, rz, h] = v

    sems = [0]

    def copy_of(src, dst, to):
        i = sems[0]
        sems[0] += 1
        return remote(src, dst, r_send.at[i], r_recv.at[i], to)

    sent = []

    class Ring:
        def __init__(self, way, pieces, far, into, a, b):
            up, down = near[way + "+"], near[way + "-"]
            self.into, self.a, self.b = into, a, b
            self.first = [copy_of(far[0], a.at[0], up), copy_of(far[1], a.at[1], down)]
            self.second = [copy_of(pieces[1], b.at[0], up), copy_of(pieces[3], b.at[1], down)]

        def begin(self):
            for c in self.first:
                c.start()

        def middle(self):
            for i in range(2):
                self.first[i].wait_recv()
                ref = self.into[i]
                ref[...] = ref[...] + self.a[i]
                self.second[i].start()

        def end(self, own, out):
            for c in self.second:
                c.wait_recv()
            out[...] = own[...] + self.b[0] + self.b[1]
            sent.extend(self.first + self.second)

    h_here = z_hi
    h_up = lax.rem(z + 1, 4) // 2

    ring0 = Ring(
        "z",
        {1: G0.at[1, h_up], 3: G0.at[1, 1 - h_up]},
        (G0.at[0, 1 - h_here, pl.ds(0, 2)], G0.at[0, 1 - h_here, pl.ds(2, 2)]),
        (G0.at[1, h_up, pl.ds(0, 2)], G0.at[1, 1 - h_up, pl.ds(2, 2)]),
        ra0, rb0,
    )
    ring1 = Ring(
        "d1",
        {1: G1.at[1], 3: G1.at[3]},
        (G1.at[2, pl.ds(0, 2)], G1.at[2, pl.ds(2, 2)]),
        (G1.at[1, pl.ds(0, 2)], G1.at[3, pl.ds(2, 2)]),
        ra1, rb1,
    )
    ring0.begin()
    ring1.begin()
    ring0.middle()
    ring1.middle()
    mine0, mine1 = G0.at[0, h_here], G1.at[0]
    ring1.end(mine1, mine1)
    ring3 = Ring(
        "d2",
        {1: G1.at[0, 1], 3: G1.at[0, 3]},
        (G1.at[0, 2, 0], G1.at[0, 2, 1]),
        (G1.at[0, 1, 0], G1.at[0, 3, 1]),
        sa1, sb1,
    )
    ring3.begin()
    ring0.end(mine0, mine0)
    ring2 = Ring(
        "d2",
        {1: G0.at[0, h_here, 1], 3: G0.at[0, h_here, 3]},
        (G0.at[0, h_here, 2, pl.ds(0, 2)], G0.at[0, h_here, 2, pl.ds(2, 2)]),
        (G0.at[0, h_here, 1, pl.ds(0, 2)], G0.at[0, h_here, 3, pl.ds(2, 2)]),
        sa0, sb0,
    )
    ring2.begin()
    ring3.middle()
    ring2.middle()
    ring3.end(G1.at[0, 0], G1.at[0, 0])
    quarter = half_piece // 2
    ring5 = Ring(
        "z",
        {1: G1.at[0, 0, 1, h_up], 3: G1.at[0, 0, 1, 1 - h_up]},
        (G1.at[0, 0, 0, 1 - h_here, pl.ds(0, quarter)], G1.at[0, 0, 0, 1 - h_here, pl.ds(quarter, quarter)]),
        (G1.at[0, 0, 1, h_up, pl.ds(0, quarter)], G1.at[0, 0, 1, 1 - h_up, pl.ds(quarter, quarter)]),
        ta1, tb1,
    )
    ring5.begin()
    ring2.end(G0.at[0, h_here, 0], G0.at[0, h_here, 0])
    ring4 = Ring(
        "d1",
        {1: G0.at[0, h_here, 0, 1], 3: G0.at[0, h_here, 0, 3]},
        (G0.at[0, h_here, 0, 2, pl.ds(0, quarter)], G0.at[0, h_here, 0, 2, pl.ds(quarter, quarter)]),
        (G0.at[0, h_here, 0, 1, pl.ds(0, quarter)], G0.at[0, h_here, 0, 3, pl.ds(quarter, quarter)]),
        ta0, tb0,
    )
    ring4.begin()
    ring5.middle()
    ring4.middle()

    factor = 1.0 / math.sqrt(TOTAL_ROWS[0])
    ring5.end(G1.at[0, 0, 0, h_here], G1.at[0, 0, 0, h_here])
    ring4.end(G0.at[0, h_here, 0, 0], G0.at[0, h_here, 0, 0])
    last = []
    for p, ref in ((1, G1.at[0, 0, 0, h_here]), (0, G0.at[0, h_here, 0, 0])):
        at = pl.multiple_of((core * 2 + p) * PIECE + z_hi * half_piece, half_piece)
        place = GO.at[pl.ds(at, half_piece), :]
        place[...] = ref[...] * factor
        for i, to in enumerate(holders):
            copy = remote(place, place, f_send.at[p * 3 + i], f_recv.at[p * 3 + i], to)
            copy.start()
            last.append(copy)
    for copy in last:
        copy.wait_recv()
    grad_out = pltpu.make_async_copy(GO, grad, out_sem.at[1])
    grad_out.start()

    for m in range(len(MSGS)):
        message(m).wait_send()
    for copy in [feat_out] + pred_out + res_out + sent + last:
        copy.wait_send()
    resid_out.wait()
    grad_out.wait()


TOTAL_ROWS = [0]


def body(features, targets, centres, widths, coefficients):
    rows, depth = features.shape
    wide = targets.shape[1]
    own = lax.axis_size("own")
    TOTAL_ROWS[0] = rows * own * lax.axis_size("grp")
    unit_rows = (depth // 128 + wide // 128) * PIECE + 8
    cols = UNITS * PIECE
    half = PIECE // 2
    n_loads = 1 + 2 * (depth // 128 + wide // 128)
    vm = pltpu.VMEM
    dma = pltpu.SemaphoreType.DMA
    scratch = [
        vm((UNITS, unit_rows, 128), F32),
        vm((1, widths.shape[0]), F32),
        vm((2, rows, depth), F32),
        vm((2 * rows, depth), BF16),
        vm((2 * rows, 2 * depth), F8),
        vm((2 * rows, 128), F32),
        vm((CHUNK, depth), BF16),
        vm((CHUNK, 2 * depth), F8),
        vm((CHUNK, wide), BF16),
        vm((2 * CHUNK, wide), F8),
        vm((8, CHUNK), F32),
        vm((2 * rows, cols), BF16),
        vm((2 * rows, 2 * cols), F8),
        vm((2 * rows, wide), F32),
        vm((rows, wide), F32),
        vm((rows, wide), F32),
        vm((rows, wide), F32),
        vm((rows, wide), F32),
        vm((wide, 2 * rows), BF16),
        vm((wide, 2 * rows), F8),
        vm((wide, 2 * rows), F8),
        vm((8, wide, CHUNK), F32),
        vm((2, 2, 4, 4, half, wide), F32),
        vm((4, 4, 2, 2, half, wide), F32),
        vm((4 * PIECE, wide), F32),
        vm((2, 2, 4, half, wide), F32),
        vm((2, 4, 4, half, wide), F32),
        vm((2, 2, half, wide), F32),
        vm((2, 4, half, wide), F32),
        vm((2, half // 2, wide), F32),
        vm((2, half, wide), F32),
        vm((2, 2, 2, 2, half, wide), F32),
        vm((2, 4, 2, 2, half, wide), F32),
        vm((2, 2, half, wide), F32),
        vm((2, 2, 2, half, wide), F32),
        vm((2, half // 2, wide), F32),
        vm((2, half, wide), F32),
        dma((n_loads,)), dma((2,)), dma((5,)), dma((5,)), dma((len(MSGS),)), dma((len(MSGS),)),
        dma((24,)), dma((24,)), dma((6,)), dma((6,)), dma((2,)),
    ]
    anywhere = pl.BlockSpec(memory_space=pl.ANY)
    return pl.pallas_call(
        main_kernel,
        out_shape=(
            jax.ShapeDtypeStruct(targets.shape, F32),
            jax.ShapeDtypeStruct(coefficients.shape, F32),
        ),
        in_specs=[anywhere] * 5,
        out_specs=(anywhere, anywhere),
        scratch_shapes=scratch,
        compiler_params=pltpu.CompilerParams(
            collective_id=0, has_side_effects=True, vmem_limit_bytes=67_043_328
        ),
        name="nystrom",
    )(features, targets, centres, widths.reshape(1, -1), coefficients)


def solution(mesh):
    return jax.shard_map(
        body,
        mesh=mesh,
        in_specs=(
            P(("grp", "own"), None),
            P(("grp", "own"), None),
            P("own", None),
            P("own"),
            P("own", None),
        ),
        out_specs=(P(("grp", "own"), None), P("own", None)),
        check_vma=False,
    )
```

```python
import functools
import math
import jax
import jax.numpy as jnp
from jax import lax
from jax.experimental import pallas as pl
from jax.experimental.pallas import tpu as pltpu
from jax.sharding import PartitionSpec as P

F32, BF16, F8 = jnp.float32, jnp.bfloat16, jnp.float8_e4m3fn
NN = (((1,), (0,)), ((), ()))
NT = (((1,), (1,)), ((), ()))
MESH = pl.DeviceIdType.MESH

PIECE = 32
CHUNK = 256
UNITS = 64
DIRS = ("d1+", "d1-", "d2+", "d2-", "z+", "z-")


def messages():
    out = []

    def add(*m):
        out.append(m)

    for r1 in range(4):
        b = (0, r1, 0)
        if r1 == 0:
            add(0, b, (0, 3, 0), None, "d1+")
            add(0, b, (0, 1, 0), None, "d1-")
        if r1 == 3:
            add(0, b, (0, 2, 0), 0, "d1+")
        if r1 == 1:
            add(0, b, (0, 2, 0), 1, "d1-")
        add(0, b, (0, r1, 3), None, "d2+")
        add(0, b, (0, r1, 1), None, "d2-")
        add(0, (0, r1, 3), (0, r1, 2), 0, "d2+")
        add(0, (0, r1, 1), (0, r1, 2), 1, "d2-")
    for r1 in range(4):
        for r2 in range(4):
            add(0, (0, r1, r2), (1, r1, r2), None, "z+" if (r1 + r2) % 2 == 0 else "z-")
    b = (0, 0, 0)
    add(1, b, (0, 0, 3), None, "d2+")
    add(1, b, (0, 0, 1), None, "d2-")
    add(1, (0, 0, 3), (0, 0, 2), 0, "d2+")
    add(1, (0, 0, 1), (0, 0, 2), 1, "d2-")
    for r2 in range(4):
        add(1, (0, 0, r2), (1, 0, r2), None, "z-" if r2 % 2 == 0 else "z+")
    for rz in range(2):
        for r2 in range(4):
            s = (rz, 0, r2)
            add(1, s, (rz, 3, r2), None, "d1+")
            add(1, s, (rz, 1, r2), None, "d1-")
            add(1, (rz, 3, r2), (rz, 2, r2), 0, "d1+")
            add(1, (rz, 1, r2), (rz, 2, r2), 1, "d1-")
    return out


FIRST = (0, 1, 36, 37, 2, 3, 40, 44, 45, 20)
SCHEDULE = (
    ((0, (15, 16, 17, 32)), (1, (6, 7, 8, 24)), (20, ()), (36, (38, 43, 56, 57)), (37, (39, 41, 48, 49)), (40, (60, 61))),
    (),
    ((2, (4, 23)), (3, (5, 21)), (44, (46,)), (45, (47,))),
    ((6, ()), (15, (11, 12, 28)), (32, ()), (43, (72, 73)), (16, (18, 35))),
    ((17, (19, 33)), (56, (58,)), (57, (59,))),
    ((24, ()), (41, (64, 65)), (7, (9, 27)), (8, (10, 25))),
    ((38, ()), (39, (42, 52, 53))),
    ((48, (50,)), (49, (51,)), (23, ()), (28, ()), (4, ()), (5, (22,))),
    ((60, (62,)), (61, (63,))),
    ((21, ()),),
    ((35, ()), (11, (13, 31)), (12, (14, 29)), (46, ()), (47, ())),
    ((18, ()), (19, (34,)), (33, ()), (42, (68, 69))),
    ((9, ()), (10, (26,))),
    ((72, (74,)), (73, (75,)), (13, ()), (14, (30,)), (58, ()), (59, ())),
    ((27, ()), (31, ()), (64, (66,)), (65, (67,))),
    (),
    ((52, (54,)), (53, (55,)), (25, ())),
    ((50, ()), (51, ()), (29, ()), (62, ()), (63, ())),
    ((68, (70,)), (69, (71,))),
    ((22, ()), (74, ()), (75, ()), (34, ()), (66, ()), (67, ())),
    ((54, ()), (55, ()), (70, ()), (71, ())),
    ((30, ()), (26, ())),
    (),
    (),
)

MSGS = messages()


def unit_order():
    place = {(0, (0, 0, 0)): 0, (1, (0, 0, 0)): 1}
    halves = {}
    for point in SCHEDULE:
        for m, _ in point:
            part, _, dst, half, _ = MSGS[m]
            seen = halves.setdefault((part, dst), set())
            seen.update((0, 1) if half is None else (half,))
            if len(seen) == 2:
                place[(part, dst)] = len(place)
    return place


EARLY = 4
PLACE = unit_order()
UNIT_AT = {v: k for k, v in PLACE.items()}
LOG2E = 1.4426950408889634
S_HI, S_LO = 4.0, 1024.0
S_K, S_KLO = 16.0, 4096.0
S_C, S_CLO = 64.0, 16384.0
S_R, S_RLO = 0.25, 64.0


def dot(a, b, dims):
    return lax.dot_general(a, b, dims, preferred_element_type=F32)


def split(v):
    hi = v.astype(BF16)
    return hi, v - hi.astype(F32)


def main_kernel(
    feat, targ, cent, wid, coef, resid, grad,
    CB, WV, FS, FH, FX, RS, CH, CX, WH, WX, MB, KH, KX, PRED, TG, PR, RES, RP,
    RTH, RTL, RTR, GT, G, GO, A1, B1, A2, B2, ZB,
    in_sem, own_sem, d_send, d_recv, g_send, g_recv, r_send, r_recv, f_send, f_recv, out_sem,
):
    rows, depth = feat.shape
    blocks = depth // 128
    unit_rows = CB.shape[1]
    tile = rows // 2
    wide = TG.shape[1]
    lane_w = wide // 128

    grp, own = lax.axis_index("grp"), lax.axis_index("own")
    core, z_hi = lax.rem(grp, 2), grp // 2
    z, x, y = z_hi * 2 + own // 16, lax.rem(own // 4, 4), lax.rem(own, 4)

    def device(d1=0, d2=0, dz=0, dcore=0):
        nx = lax.rem(x + 4 + d1 * (1 - core) + d2 * core, 4)
        ny = lax.rem(y + 4 + d1 * core + d2 * (1 - core), 4)
        nz = lax.rem(z + 4 + dz, 4)
        nc = lax.rem(core + dcore, 2)
        return ((nz // 2) * 2 + nc, lax.rem(nz, 2) * 16 + nx * 4 + ny)

    near = {
        "d1+": device(d1=1), "d1-": device(d1=-1),
        "d2+": device(d2=1), "d2-": device(d2=-1),
        "z+": device(dz=1), "z-": device(dz=-1),
    }
    sibling = device(dcore=1)
    across = device(dz=2)

    def remote(src, dst, send, recv, to):
        return pltpu.make_async_remote_copy(
            src_ref=src, dst_ref=dst, send_sem=send, recv_sem=recv, device_id=to, device_id_type=MESH
        )

    loads = []

    def load(src, dst):
        copy = pltpu.make_async_copy(src, dst, in_sem.at[len(loads)])
        copy.start()
        loads.append(copy)
        return copy

    load(wid, WV)
    for p in range(2):
        first = pl.multiple_of((core * 2 + p) * PIECE, PIECE)
        for b in range(blocks):
            load(
                cent.at[pl.ds(first, PIECE), pl.ds(b * 128, 128)],
                CB.at[p, pl.ds(b * PIECE, PIECE), :],
            )
        for b in range(lane_w):
            load(
                coef.at[pl.ds(first, PIECE), pl.ds(b * 128, 128)],
                CB.at[p, pl.ds((blocks + b) * PIECE, PIECE), :],
            )
    feat_in = pltpu.make_async_copy(feat, FS.at[0], own_sem.at[0])
    feat_in.start()
    targ_in = pltpu.make_async_copy(targ, TG, own_sem.at[1])
    targ_in.start()

    barrier = pltpu.get_barrier_semaphore()
    peers = list(near.values()) + [sibling, across]
    for to in peers:
        pl.semaphore_signal(barrier, inc=1, device_id=to, device_id_type=MESH)
    for copy in loads:
        copy.wait()

    row_i = lax.broadcasted_iota(jnp.int32, (PIECE, 128), 0)
    lane_i = lax.broadcasted_iota(jnp.int32, (PIECE, 128), 1)
    eye = (row_i == lane_i).astype(F32)
    meta_row = lax.broadcasted_iota(jnp.int32, (8, 128), 0)
    for p in range(2):
        sq = jnp.zeros((PIECE, 128), F32)
        for b in range(blocks):
            v = CB[p, b * PIECE : (b + 1) * PIECE, :]
            sq = sq + v * v
        norm = jnp.sum(sq, axis=1, keepdims=True)
        picked = jnp.where(lane_i == row_i + (core * 2 + p) * PIECE, WV[...], 0.0)
        width = jnp.sum(picked, axis=1, keepdims=True)
        scale = (-0.5 * LOG2E) / width
        norm = jnp.sum(norm * eye, axis=0, keepdims=True)
        scale = jnp.sum(scale * eye, axis=0, keepdims=True)
        CB[p, unit_rows - 8 : unit_rows, :] = jnp.where(
            meta_row == 0, scale, jnp.where(meta_row == 1, norm, 0.0)
        )
    pl.semaphore_wait(barrier, len(peers))

    cut = (unit_rows // 16) * 8
    spans = {None: (0, unit_rows), 0: (0, cut), 1: (cut, unit_rows - cut)}

    def message(m):
        part, src, dst, half, way = MSGS[m]
        at, size = spans[half]
        return remote(
            CB.at[PLACE[(part, src)], pl.ds(at, size), :],
            CB.at[PLACE[(part, dst)], pl.ds(at, size), :],
            g_send.at[m], g_recv.at[m], near[way],
        )

    def service(point):
        for m, onward in point:
            message(m).wait_recv()
            for n in onward:
                message(n).start()

    for m in FIRST:
        message(m).start()
    share = rows // 4
    feat_out = [
        remote(
            feat.at[pl.ds(i * share, share), :], FS.at[1, pl.ds(i * share, share), :],
            d_send.at[i], d_recv.at[i], sibling,
        )
        for i in range(4)
    ]
    for copy in feat_out:
        copy.start()

    def prepare_rows(which, first, count):
        base = which * rows
        step = min(128, count)

        @pl.loop(0, count // step)
        def _(i):
            r = pl.multiple_of(first + i * step, step)
            v = FS[which, pl.ds(r, step), :]
            hi, lo = split(v)
            to = pl.ds(base + r, step)
            FH[to, :] = hi
            FX[to, 0:depth] = (v * S_HI).astype(F8)
            FX[to, depth : 2 * depth] = (lo * S_LO).astype(F8)
            RS[to, :] = jnp.broadcast_to(jnp.sum(v * v, axis=1, keepdims=True), (step, 128))

    def prepare_chunk(k):
        units = range(8 * k, 8 * k + 8)
        for b in range(blocks):
            v = jnp.concatenate([CB[u, b * PIECE : (b + 1) * PIECE, :] for u in units], axis=0)
            hi, lo = split(v)
            CH[:, b * 128 : (b + 1) * 128] = hi
            CX[:, b * 128 : (b + 1) * 128] = (lo * S_LO).astype(F8)
            CX[:, depth + b * 128 : depth + (b + 1) * 128] = (v * S_HI).astype(F8)
        for b in range(lane_w):
            at = (blocks + b) * PIECE
            v = jnp.concatenate([CB[u, at : at + PIECE, :] for u in units], axis=0)
            hi, lo = split(v)
            WH[:, b * 128 : (b + 1) * 128] = hi
            WX[0:CHUNK, b * 128 : (b + 1) * 128] = (lo * S_CLO).astype(F8)
            WX[CHUNK : 2 * CHUNK, b * 128 : (b + 1) * 128] = (v * S_C).astype(F8)
        for h in range(2):
            total = CB[8 * k + 4 * h, unit_rows - 8 : unit_rows, :]
            for j in range(1, 4):
                meta = CB[8 * k + 4 * h + j, unit_rows - 8 : unit_rows, :]
                total = total + pltpu.roll(meta, j * PIECE, 1)
            MB[:, h * 128 : (h + 1) * 128] = total

    def compute(k, base, size):
        r = pl.ds(base, size)
        cross = dot(FH[r, :], CH[...], NT)
        fine = dot(FX[r, :], CX[...], NT)
        norm = RS[r, :]
        norm = jnp.concatenate([norm, norm], axis=1)
        s = (norm + MB[1:2, :]) - 2.0 * cross - fine * (2.0 / (S_HI * S_LO))
        kern = jnp.exp2(s * MB[0:1, :])
        hi, lo = split(kern)
        KH[r, k * CHUNK : (k + 1) * CHUNK] = hi
        both = jnp.concatenate([(kern * S_K).astype(F8), (lo * S_KLO).astype(F8)], axis=1)
        KX[r, 2 * k * CHUNK : 2 * (k + 1) * CHUNK] = both
        term = dot(hi, WH[...], NN) + dot(both, WX[...], NN) * (1.0 / (S_K * S_CLO))
        if k == 0:
            PRED[r, :] = term
        else:
            PRED[r, :] = PRED[r, :] + term

    feat_in.wait()
    prepare_rows(0, 0, rows)
    for i in range(4):
        feat_out[i].wait_recv()
        prepare_rows(1, i * share, share)
    pred_out = [
        remote(
            PRED.at[pl.ds(rows + i * tile, tile), :], PR.at[pl.ds(i * tile, tile), :],
            d_send.at[4 + i], d_recv.at[4 + i], sibling,
        )
        for i in range(2)
    ]
    for k in range(8):
        before, after0, after1 = SCHEDULE[3 * k : 3 * k + 3]
        service(before)
        prepare_chunk(k)
        if k < 7:

            @pl.loop(0, 2)
            def _(s):
                compute(k, pl.multiple_of(s * rows, rows), rows)
                for at, point in ((0, after0), (1, after1)):
                    if point:
                        pl.when(s == at)(functools.partial(service, point))
        else:
            for i in range(2):
                compute(k, rows + i * tile, tile)
                pred_out[i].start()
            service(after0)
            compute(k, 0, rows)
            service(after1)

    def factors(v, at):
        t = v.T
        hi, lo = split(t)
        RTH[:, at : at + tile] = hi
        RTL[:, at : at + tile] = (lo * S_RLO).astype(F8)
        RTR[:, at : at + tile] = (t * S_R).astype(F8)

    targ_in.wait()
    res_out = []
    for i in range(2):
        part = pl.ds(i * tile, tile)
        pred_out[i].wait_recv()
        v = PRED[part, :] + PR[part, :] - TG[part, :]
        RES[part, :] = v
        copy = remote(RES.at[part, :], RP.at[part, :], d_send.at[6 + i], d_recv.at[6 + i], sibling)
        copy.start()
        res_out.append(copy)
        factors(v, i * tile)
    resid_out = pltpu.make_async_copy(RES, resid, out_sem.at[0])
    resid_out.start()

    def gradient_term(base, size, k):
        r = pl.ds(base, size)
        c0, c1, c2 = k * CHUNK, 2 * k * CHUNK, (2 * k + 1) * CHUNK
        term = dot(RTH[:, r], KH[r, c0 : c0 + CHUNK], NN)
        fine = dot(RTL[:, r], KX[r, c1 : c1 + CHUNK], NN) + dot(RTR[:, r], KX[r, c2 : c2 + CHUNK], NN)
        return term + fine * (1.0 / (S_RLO * S_K))

    ways = (("d2", "d1"), ("d1", "d2"))

    def ring_copies(part, level):
        first, second = (A1, B1) if level == 0 else (A2, B2)
        pieces = G.at[part] if level == 0 else G.at[part, 0]
        n = 2 if level == 0 else 1
        up, down = (near[ways[part][level] + sign] for sign in "+-")
        low, high = (pl.ds(0, n), pl.ds(n, n))
        out = []
        for i, (a, span, dst, at, to) in enumerate((
            (2, low, first, None, up), (2, high, first, None, down),
            (1, high, second, high, up), (3, low, second, low, down),
            (1, low, second, low, up), (3, high, second, high, down),
        )):
            side = i % 2
            src = pieces.at[a, span]
            if at is None:
                target = dst.at[part, side] if level == 0 else dst.at[part, pl.ds(side, 1)]
            else:
                target = dst.at[part, side, at]
            sem = part * 12 + level * 6 + i
            out.append((src, target, sem, to))
        return out

    rings = {(p, v): ring_copies(p, v) for p in range(2) for v in range(2)}

    def ring_copy(p, v, i):
        src, target, sem, to = rings[(p, v)][i]
        return remote(src, target, r_send.at[sem], r_recv.at[sem], to)

    def send_unit(part, a, b, rz):
        at = {2: 0 if b < 2 else 1, 1: 2 if b >= 2 else None, 3: 3 if b < 2 else None}.get(a)
        if at is None:
            return
        _, _, sem, to = rings[(part, 0)][at]
        target = A1.at[part, at, b % 2, rz] if a == 2 else B1.at[part, at - 2, b, rz]
        remote(G.at[part, a, b, rz], target, r_send.at[sem], r_recv.at[sem], to).start()

    far = [sum(UNIT_AT[8 * k + j][1][2 - UNIT_AT[8 * k + j][0]] == 2 for j in range(8)) for k in range(8)]
    order = sorted(range(8), key=lambda k: -far[k])
    for i, k in enumerate(order[:EARLY]):
        GT[i] = gradient_term(0, rows, k)
    for i in range(2):
        res_out[i].wait_recv()
        factors(RP[i * tile : (i + 1) * tile, :], rows + i * tile)
    for i, k in enumerate(order):
        t = GT[i] + gradient_term(rows, rows, k) if i < EARLY else gradient_term(0, 2 * rows, k)
        t = t.T
        for j in range(8):
            part, (rz, r1, r2) = UNIT_AT[8 * k + j]
            a, b = (r2, r1) if part == 0 else (r1, r2)
            G[part, a, b, rz] = t[j * PIECE : (j + 1) * PIECE, :]
            send_unit(part, a, b, rz)

    def ring_middle(p, v):
        first = A1 if v == 0 else A2
        n = 2 if v == 0 else 1
        pieces = G.at[p] if v == 0 else G.at[p, 0]
        for side, a, span in ((0, 1, slice(0, n)), (1, 3, slice(n, 2 * n))):
            ring_copy(p, v, side).wait_recv()
            got = first[p, side] if v == 0 else first[p, side : side + 1]
            pieces[a, span] = pieces[a, span] + got
            ring_copy(p, v, 4 + side).start()

    def ring_end(p, v):
        second = B1 if v == 0 else B2
        pieces = G.at[p] if v == 0 else G.at[p, 0]
        for i in range(2, 6):
            ring_copy(p, v, i).wait_recv()
        pieces[0] = pieces[0] + second[p, 0] + second[p, 1]

    ring_middle(0, 0)
    ring_middle(1, 0)
    for p in range(2):
        ring_end(p, 0)
        for i in range(4):
            ring_copy(p, 1, i).start()
    ring_middle(0, 1)
    ring_middle(1, 1)

    z_copies = []
    for p in range(2):
        ring_end(p, 1)
        for i, (rz, to) in enumerate(((0, across), (1, near["z+"]), (1, near["z-"]))):
            copy = remote(G.at[p, 0, 0, rz], ZB.at[i, p], f_send.at[3 * p + i], f_recv.at[3 * p + i], to)
            copy.start()
            z_copies.append(copy)
    factor = 1.0 / math.sqrt(TOTAL_ROWS[0])
    last = []
    for p in range(2):
        for copy in z_copies[3 * p : 3 * p + 3]:
            copy.wait_recv()
        at = pl.multiple_of((core * 2 + p) * PIECE, PIECE)
        place = GO.at[pl.ds(at, PIECE), :]
        place[...] = ((G[p, 0, 0, 0] + ZB[0, p]) + (ZB[1, p] + ZB[2, p])) * factor
        copy = remote(place, place, f_send.at[6 + p], f_recv.at[6 + p], sibling)
        copy.start()
        last.append(copy)
    for copy in last:
        copy.wait_recv()
    grad_out = pltpu.make_async_copy(GO, grad, out_sem.at[1])
    grad_out.start()

    for m in range(len(MSGS)):
        message(m).wait_send()
    for p in range(2):
        for v in range(2):
            for i in range(6):
                ring_copy(p, v, i).wait_send()
    for copy in feat_out + pred_out + res_out + z_copies + last:
        copy.wait_send()
    resid_out.wait()
    grad_out.wait()


TOTAL_ROWS = [0]


def hand_over(res_in, grad_in, res_out, grad_out, held, held_grad, sem_in, sem_out):
    parts = held.shape[0]
    size = held.shape[1]
    pairs = [
        (res_in.at[pl.ds(i * size, size), :], held.at[i], res_out.at[pl.ds(i * size, size), :])
        for i in range(parts)
    ] + [(grad_in, held_grad, grad_out)]
    copies = [pltpu.make_async_copy(a, v, sem_in.at[i]) for i, (a, v, _) in enumerate(pairs)]
    for c in copies:
        c.start()
    backs = [pltpu.make_async_copy(v, b, sem_out.at[i]) for i, (_, v, b) in enumerate(pairs)]
    for c, b in zip(copies, backs):
        c.wait()
        b.start()
    for b in backs:
        b.wait()


def body(features, targets, centres, widths, coefficients):
    rows, depth = features.shape
    wide = targets.shape[1]
    own = lax.axis_size("own")
    TOTAL_ROWS[0] = rows * own * lax.axis_size("grp")
    unit_rows = (depth // 128 + wide // 128) * PIECE + 8
    cols = UNITS * PIECE
    n_loads = 1 + 2 * (depth // 128 + wide // 128)
    vm = pltpu.VMEM
    dma = pltpu.SemaphoreType.DMA
    scratch = [
        vm((UNITS, unit_rows, 128), F32),
        vm((1, widths.shape[0]), F32),
        vm((2, rows, depth), F32),
        vm((2 * rows, depth), BF16),
        vm((2 * rows, 2 * depth), F8),
        vm((2 * rows, 128), F32),
        vm((CHUNK, depth), BF16),
        vm((CHUNK, 2 * depth), F8),
        vm((CHUNK, wide), BF16),
        vm((2 * CHUNK, wide), F8),
        vm((8, CHUNK), F32),
        vm((2 * rows, cols), BF16),
        vm((2 * rows, 2 * cols), F8),
        vm((2 * rows, wide), F32),
        vm((rows, wide), F32),
        vm((rows, wide), F32),
        vm((rows, wide), F32),
        vm((rows, wide), F32),
        vm((wide, 2 * rows), BF16),
        vm((wide, 2 * rows), F8),
        vm((wide, 2 * rows), F8),
        vm((EARLY, wide, CHUNK), F32),
        vm((2, 4, 4, 2, PIECE, wide), F32),
        vm((4 * PIECE, wide), F32),
        vm((2, 2, 2, 2, PIECE, wide), F32),
        vm((2, 2, 4, 2, PIECE, wide), F32),
        vm((2, 2, PIECE, wide), F32),
        vm((2, 2, 2, PIECE, wide), F32),
        vm((3, 2, PIECE, wide), F32),
        dma((n_loads,)), dma((2,)), dma((8,)), dma((8,)), dma((len(MSGS),)), dma((len(MSGS),)),
        dma((24,)), dma((24,)), dma((8,)), dma((8,)), dma((2,)),
    ]
    anywhere = pl.BlockSpec(memory_space=pl.ANY)
    residual, gradient = pl.pallas_call(
        main_kernel,
        out_shape=(
            jax.ShapeDtypeStruct(targets.shape, F32),
            jax.ShapeDtypeStruct(coefficients.shape, F32),
        ),
        in_specs=[anywhere] * 5,
        out_specs=(anywhere, anywhere),
        scratch_shapes=scratch,
        compiler_params=pltpu.CompilerParams(
            collective_id=0, has_side_effects=True, vmem_limit_bytes=67_043_328
        ),
        name="nystrom",
    )(features, targets, centres, widths.reshape(1, -1), coefficients)
    return pl.pallas_call(
        hand_over,
        out_shape=(
            jax.ShapeDtypeStruct(targets.shape, F32),
            jax.ShapeDtypeStruct(coefficients.shape, F32),
        ),
        in_specs=[anywhere] * 2,
        out_specs=(anywhere, anywhere),
        scratch_shapes=[
            vm((4, rows // 4, wide), F32), vm(coefficients.shape, F32), dma((5,)), dma((5,)),
        ],
        name="hand_over",
    )(residual, gradient)


def solution(mesh):
    return jax.shard_map(
        body,
        mesh=mesh,
        in_specs=(
            P(("grp", "own"), None),
            P(("grp", "own"), None),
            P("own", None),
            P("own"),
            P("own", None),
        ),
        out_specs=(P(("grp", "own"), None), P("own", None)),
        check_vma=False,
    )
```
